16 devices in a mesh: dp: 4 (over y, z, core), ep: 4 (over x).
Axes of the slice: x: 4, y: 2, z: 1, core: 2. Of those that a mesh axis runs over, the one named last changes fastest.
The devices are a block of a 4x4x4 slice.
Arguments:
- x: bfloat16 [4, 4, 384, 5120], P('dp', 'ep'), parts along dimension 0
- expert: int32 [4, 4, 384, 8], P('dp', 'ep'), parts along dimension 0
- slot: int32 [4, 4, 384, 8], P('dp', 'ep'), parts along dimension 0
- gate: float32 [4, 4, 384, 8], P('dp', 'ep'), parts along dimension 0
- w_gate: bfloat16 [40, 5120, 1536], P('ep')
- w_up: bfloat16 [40, 5120, 1536], P('ep')
- w_down: bfloat16 [40, 1536, 5120], P('ep')
- s_gate: bfloat16 [5120, 1536], replicated
- s_up: bfloat16 [5120, 1536], replicated
- s_down: bfloat16 [1536, 5120], replicated
Outputs:
- y: bfloat16 [4, 4, 384, 5120], P('dp', 'ep'), parts along dimension 0
There are 4 independent parts. The reference program is written for one: setup_inputs(seed, part) draws one part's arguments, and reference() takes and returns one part's arrays. A program takes and returns all parts, laid end to end along the dimension named above; an argument that names none is the same for every part.
All inputs are finite; a program needn't handle non-finite values.
Results may differ from the reference program's by a relative error of at most 0.009.
Values are sent between devices in bfloat16 or wider.
A program may use at most 1.5 GiB of HBM per device.

```python
import jax
import jax.numpy as jnp

MEMBERS = 4
TOKENS = 384
D = 5120
FF = 1536
TOP = 8
EXPERTS = 40
SHARED_FF = 1536
SLOTS = 5 * TOKENS * TOP // (4 * EXPERTS)


def setup_inputs(seed: int = 0, part: int = 0) -> dict:
    own, k1, k2, k3, k4, k5, k6 = jax.random.split(jax.random.key(seed), 7)
    kx, ke, kl, kg = jax.random.split(jax.random.fold_in(own, part), 4)
    devices = (1, MEMBERS)
    place = jax.random.permutation(kl, jnp.arange(EXPERTS, dtype=jnp.uint32))
    slow = ((EXPERTS + (9 * place) % EXPERTS) << ((9 * place) // EXPERTS)) // EXPERTS
    wait = (jax.random.bits(ke, (*devices, TOKENS, EXPERTS), jnp.uint32) >> 10) * slow
    expert = jnp.argsort(wait, axis=-1)[..., :TOP].astype(jnp.int32)
    chosen = jax.nn.one_hot(expert, EXPERTS, dtype=jnp.int32)
    in_line = jnp.cumsum(chosen.reshape(*devices, TOKENS * TOP, EXPERTS), axis=2) - 1
    slot = jnp.sum(in_line.reshape(chosen.shape) * chosen, axis=-1)

    def one(key, rows, columns):
        return (jax.random.normal(key, (rows, columns), jnp.float32) * rows**-0.5).astype(jnp.bfloat16)

    def weights(key, rows, columns):
        return jax.lax.map(lambda k: one(k, rows, columns), jax.random.split(key, EXPERTS))

    return {
        "x": jax.random.normal(kx, (*devices, TOKENS, D), jnp.float32).astype(jnp.bfloat16),
        "expert": expert,
        "slot": slot,
        "gate": jax.nn.softmax(jax.random.normal(kg, expert.shape, jnp.float32)),
        "w_gate": weights(k1, D, FF),
        "w_up": weights(k2, D, FF),
        "w_down": weights(k3, FF, D),
        "s_gate": one(k4, D, SHARED_FF),
        "s_up": one(k5, D, SHARED_FF),
        "s_down": one(k6, SHARED_FF, D),
    }


def einsum(form, a, b):
    return jnp.einsum(form, a.astype(jnp.float32), b.astype(jnp.float32))


def for_all(x, s_gate, s_up, s_down):
    h = jax.nn.silu(einsum("...d,df->...f", x, s_gate)) * einsum("...d,df->...f", x, s_up)
    return einsum("...f,fd->...d", h.astype(jnp.bfloat16), s_down)


def reference(x, expert, slot, gate, w_gate, w_up, w_down, s_gate, s_up, s_down):
    to_expert = jax.nn.one_hot(expert, EXPERTS, dtype=jnp.bfloat16)
    to_slot = jax.nn.one_hot(slot, SLOTS, dtype=jnp.bfloat16)
    weighted = to_expert * gate[..., None].astype(jnp.bfloat16)
    dispatch = einsum("abtke,abtkc->abtec", to_expert, to_slot).astype(jnp.bfloat16)
    combine = einsum("abtke,abtkc->abtec", weighted, to_slot).astype(jnp.bfloat16)
    z = einsum("abtec,abtd->aebcd", dispatch, x).astype(jnp.bfloat16)
    h = jax.nn.silu(einsum("aebcd,edf->aebcf", z, w_gate))
    h = (h * einsum("aebcd,edf->aebcf", z, w_up)).astype(jnp.bfloat16)
    out = einsum("aebcf,efd->aebcd", h, w_down).astype(jnp.bfloat16)
    y = einsum("abtec,aebcd->abtd", combine, out)
    return (y + for_all(x, s_gate, s_up, s_down)).astype(jnp.bfloat16)
```

```python
import jax
import jax.numpy as jnp
from jax import lax
from jax.experimental import pallas as pl
from jax.experimental.pallas import tpu as pltpu
from jax.sharding import PartitionSpec as P

F32, BF16 = jnp.float32, jnp.bfloat16
MESH = pl.DeviceIdType.MESH
VMEM_BYTES = 67_000_000
X_COLUMNS, F_COLUMNS, X_RING = 512, 1536, 2
Y_COLUMNS, Y_RING, LAG = 512, 3, 3


def dot(a, b):
    return jnp.dot(a, b, preferred_element_type=F32)


def ring(members):
    me = lax.axis_index("ep")
    return me, lax.rem(me + 1, members), lax.rem(me + members - 1, members), lax.rem(me + 2, members)


def greet(*devices):
    barrier = pltpu.get_barrier_semaphore()
    for device in devices:
        pl.semaphore_signal(barrier, inc=1, device_id={"ep": device}, device_id_type=MESH)
    pl.semaphore_wait(barrier, len(devices))


def remote(src, dst, send, recv, device):
    return pltpu.make_async_remote_copy(
        src_ref=src, dst_ref=dst, send_sem=send, recv_sem=recv, device_id={"ep": device}, device_id_type=MESH
    )


def block(i, size):
    return pl.ds(pl.multiple_of(i * size, size), size)


def gather_kernel(
    members, x, meta, w_gate, w_up, s_gate, s_up, h, hs, xg, metas,
    acc_g, acc_u, xbuf, z, onehot, wbuf, hbuf, mbuf,
    s1s, s1r, s2s, s2r, ms, mr, wsem, xsem, hsem,
):
    (tokens, d), (local, rows, width) = x.shape, z.shape
    slots, half, chunks = rows // members, tokens // 2, d // width
    depth, fb = wbuf.shape[0], wbuf.shape[3]
    ff, hw, top = w_gate.shape[2], hbuf.shape[2], meta.shape[0] // 2
    nf = ff // fb
    head, steps = chunks * nf, local * nf
    me, right, left, across = ring(members)
    sides = (right, left)
    greet(right, left, across)

    def first(k, side):
        return remote(x.at[:, block(k, width)], xg.at[side, :, block(k, width)], s1s.at[k, side], s1r.at[k, side], sides[side])

    def second(k, side):
        part = pl.ds(side * half, half)
        return remote(
            xg.at[side, part, block(k, width)], xg.at[2, part, block(k, width)], s2s.at[k, side], s2r.at[k, side], sides[side]
        )

    def tell(i):
        return remote(meta, mbuf.at[i], ms.at[i], mr.at[i], (right, left, across)[i])

    def relay(k):
        for side in range(2):
            first(k, side).wait_recv()
        for side in range(2):
            second(k, side).start()

        @pl.when(k + 1 < chunks)
        def _():
            for side in range(2):
                first(k + 1, side).start()

    def weights(g, slot, start):
        def copies(gate, up):
            for i, src in enumerate((gate, up)):
                copy = pltpu.make_async_copy(src, wbuf.at[slot, i], wsem.at[slot, i])
                copy.start() if start else copy.wait()

        if not start:
            return copies(s_gate.at[:width, :fb], s_up.at[:width, :fb])

        @pl.when(g < head)
        def _():
            k, f = g // nf, g % nf
            copies(*(s.at[block(k, width), block(f, fb)] for s in (s_gate, s_up)))

        @pl.when((g >= head) & (g < head + chunks * steps))
        def _():
            k, i = (g - head) // steps, (g - head) % steps
            copies(*(w.at[i // nf, block(k, width), block(i % nf, fb)] for w in (w_gate, w_up)))

    def tokens_in(k, source, slot):
        src = x if source == 0 else xg.at[source - 1]
        return pltpu.make_async_copy(src.at[:, block(k, width)], xbuf.at[slot], xsem.at[slot])

    def put(dst, p):
        return pltpu.make_async_copy(hbuf.at[p], dst, hsem.at[p])

    def activate(zz, i, slot, dst, last, wait):
        for j in range(fb // hw):
            part = pl.ds(j * hw, hw)
            g, u = acc_g[i, :, part], acc_u[i, :, part]
            if last:
                g += dot(zz, wbuf[slot, 0, :, part])
                u += dot(zz, wbuf[slot, 1, :, part])
            v = (jax.nn.silu(g) * u).astype(BF16)
            p = (i % nf) * (fb // hw) + j
            if wait:
                put(hs.at[:, pl.ds(0, hw)], p).wait()
            hbuf[p] = v
            put(dst.at[:, block(p, hw)], p).start()

    for side in range(2):
        first(0, side).start()
    for i in range(members - 1):
        tell(i).start()
    for g in range(depth - 1):
        weights(jnp.int32(g), g, True)
    for k in range(members - 1):
        tokens_in(k, 0, k).start()

    @pl.loop(0, chunks)
    def _(k):
        slot_x = k % members

        @pl.when(k + members - 1 < chunks)
        def _():
            tokens_in(k + members - 1, 0, (k + members - 1) % members).start()

        @pl.when(k == (2 * chunks) // 3)
        def _():
            relay(0)

        tokens_in(k, 0, slot_x).wait()
        for f in range(nf):
            g = k * nf + f
            slot = g % depth
            weights(g, slot, False)
            weights(g + depth - 1, (g + depth - 1) % depth, True)

            @pl.when(k == 0)
            def _():
                acc_g[f] = dot(xbuf[slot_x], wbuf[slot, 0])
                acc_u[f] = dot(xbuf[slot_x], wbuf[slot, 1])

            @pl.when(k > 0)
            def _():
                acc_g[f] += dot(xbuf[slot_x], wbuf[slot, 0])
                acc_u[f] += dot(xbuf[slot_x], wbuf[slot, 1])

    for f in range(nf):
        activate(None, f, 0, hs, False, False)

    for i in range(members - 1):
        tell(i).wait_recv()
    for r in range(members):
        at = (meta if r == 0 else mbuf.at[r - 1])[:top, :] - (me * local * slots).astype(F32)

        @pl.loop(0, local)
        def _(e):
            row = (lax.broadcasted_iota(jnp.int32, (slots, tokens), 0) + e * slots).astype(F32)
            hit = at[0:1] == row
            for j in range(1, top):
                hit |= at[j : j + 1] == row
            onehot[r, block(e, slots), :] = jnp.where(hit, 1.0, 0.0).astype(BF16)

    for side in range(2):
        second(jnp.int32(0), side).wait_recv()
    for r in range(members):
        tokens_in(0, r, r).start()

    @pl.loop(0, chunks)
    def _(k):
        for r in range(members):
            tokens_in(k, r, r).wait()
        for r in range(members):
            for j in range(2):
                n = local // 2
                v = dot(onehot[r, pl.ds(j * n * slots, n * slots), :], xbuf[r]).astype(BF16)
                z[j * n : (j + 1) * n, r * slots : (r + 1) * slots, :] = v.reshape(n, slots, width)

        @pl.loop(0, steps)
        def _(i):
            g = head + k * steps + i
            slot = g % depth

            @pl.when((i == (2 * steps) // 5) & (k + 1 < chunks))
            def _():
                relay(k + 1)

            @pl.when((i == (4 * steps) // 5) & (k + 1 < chunks))
            def _():
                for side in range(2):
                    second(k + 1, side).wait_recv()
                for r in range(members):
                    tokens_in(k + 1, r, r).start()

            weights(g, slot, False)
            weights(g + depth - 1, (g + depth - 1) % depth, True)
            e = i // nf

            @pl.when(k == 0)
            def _():
                acc_g[i] = dot(z[e], wbuf[slot, 0])
                acc_u[i] = dot(z[e], wbuf[slot, 1])

            @pl.when((k > 0) & (k < chunks - 1))
            def _():
                acc_g[i] += dot(z[e], wbuf[slot, 0])
                acc_u[i] += dot(z[e], wbuf[slot, 1])

            @pl.when(k == chunks - 1)
            def _():
                activate(z[e], i, slot, h.at[e], True, True)

    for p in range(ff // hw):
        put(hs.at[:, pl.ds(0, hw)], p).wait()
    for i in range(members - 1):
        tell(i).wait_send()

    @pl.loop(0, chunks)
    def _(k):
        for side in range(2):
            first(k, side).wait_send()
            second(k, side).wait_send()

    metas[0] = meta[...]
    metas[1:] = mbuf[...]


def scatter_kernel(
    members, h, hs, metas, w_down, s_down, y,
    hbuf, comb, wbuf, outs, pend, own, abuf, bbuf, arecv, brecv, ybuf,
    hsem, wsem, a_s, a_r, b_s, b_r, ysem,
):
    (local, rows, ff), width, d = h.shape, wbuf.shape[3], y.shape[1]
    tokens, top = hs.shape[0], metas.shape[2] // 2
    slots, half, chunks = rows // members, tokens // 2, d // width
    depth, pairs, lag = wbuf.shape[0], local // 2, own.shape[0] - 1
    steps = pairs + 1
    me, right, left, _ = ring(members)
    sides = (right, left)
    greet(right, left)

    def weights(g, slot, start):
        n, p = g // steps, g % steps

        def go(copy):
            copy.start() if start else copy.wait()

        @pl.when((p < pairs) & (n < chunks))
        def _():
            for i in range(2):
                go(pltpu.make_async_copy(w_down.at[2 * p + i, :, block(n, width)], wbuf.at[slot, i], wsem.at[slot, i]))

        @pl.when((p == pairs) & (n < chunks))
        def _():
            go(pltpu.make_async_copy(s_down.at[:, block(n, width)], wbuf.at[slot, 0], wsem.at[slot, 0]))

    def take(e):
        return pltpu.make_async_copy(h.at[e], hbuf.at[e], hsem.at[e])

    def across(n, side):
        return remote(abuf.at[n % 2, pl.ds(side * half, half)], arecv.at[n, side], a_s.at[n, side], a_r.at[n, side], sides[side])

    def beside(n, side):
        return remote(bbuf.at[n % 2, side], brecv.at[n, side], b_s.at[n, side], b_r.at[n, side], sides[side])

    def put(n):
        return pltpu.make_async_copy(ybuf.at[n % 2], y.at[:, block(n, width)], ysem.at[n % 2])

    for e in range(local):
        take(e).start()
    for g in range(depth - 1):
        weights(jnp.int32(g), g, True)

    base = (me * local * slots).astype(F32)
    for r in range(members):

        @pl.loop(0, tokens // 96)
        def _(t):
            part = block(t, 96)
            at, gate = metas[r, part, :top] - base, metas[r, part, top:]
            row = lax.broadcasted_iota(jnp.int32, (96, local * slots), 1).astype(F32)
            v = jnp.zeros(row.shape, F32)
            for j in range(top):
                v = jnp.where(at[:, j : j + 1] == row, gate[:, j : j + 1], v)
            comb[r, part, :] = v.astype(BF16)

    def pair(n, p):
        g = n * steps + p
        slot = g % depth

        @pl.when(n == 0)
        def _():
            for i in range(2):
                take(2 * p + i).wait()

        weights(g, slot, False)
        weights(g + depth - 1, (g + depth - 1) % depth, True)
        for i in range(2):
            v = dot(hbuf[2 * p + i], wbuf[slot, i]).astype(BF16)
            outs[:, 2 * p + i] = v.reshape(members, slots, width)

    @pl.loop(0, chunks + lag)
    def _(n):
        @pl.when(n < chunks)
        def _():
            @pl.loop(0, (pairs + 1) // 2)
            def _(p):
                pair(n, p)

        @pl.when((n >= 1) & (n <= chunks))
        def _():
            m = n - 1
            for side in range(2):
                across(m, side).wait_recv()
            for side in range(2):

                @pl.when(m >= 2)
                def _():
                    beside(m - 2, side).wait_send()

                mine, other = pl.ds(side * half, half), pl.ds((1 - side) * half, half)
                v = pend[m % 2, side, mine] + arecv[m, side].astype(F32)
                bbuf[m % 2, side, mine] = v.astype(BF16)
                bbuf[m % 2, side, other] = pend[m % 2, side, other].astype(BF16)
                beside(m, side).start()

        @pl.when(n < chunks)
        def _():
            @pl.loop((pairs + 1) // 2, pairs)
            def _(p):
                pair(n, p)

            def term(r):
                return dot(comb[r], outs[r].reshape(local * slots, width))

            @pl.when(n >= 2)
            def _():
                for side in range(2):
                    across(n - 2, side).wait_send()

            abuf[n % 2] = term(3).astype(BF16)
            for side in range(2):
                across(n, side).start()
            g = n * steps + pairs
            slot = g % depth
            weights(g, slot, False)
            weights(g + depth - 1, (g + depth - 1) % depth, True)
            pend[n % 2, 0] = term(2)
            pend[n % 2, 1] = term(1)
            own[n % (lag + 1)] = term(0) + dot(hs[...], wbuf[slot, 0])

        @pl.when(n >= lag)
        def _():
            q = n - lag
            for side in range(2):
                beside(q, side).wait_recv()

            @pl.when(q >= 2)
            def _():
                put(q - 2).wait()

            ybuf[q % 2] = (own[q % (lag + 1)] + brecv[q, 0].astype(F32) + brecv[q, 1].astype(F32)).astype(BF16)
            put(q).start()

    for n in range(chunks - 2, chunks):
        put(jnp.int32(n)).wait()
        for side in range(2):
            across(jnp.int32(n), side).wait_send()
            beside(jnp.int32(n), side).wait_send()


def gather(members, x, meta, w_gate, w_up, s_gate, s_up, slots):
    (tokens, d), (local, _, ff) = x.shape, w_gate.shape
    rows, chunks, hw = members * slots, d // X_COLUMNS, ff // 2
    steps = local * ff // F_COLUMNS
    hbm, vmem = pl.BlockSpec(memory_space=pl.ANY), pl.BlockSpec(memory_space=pltpu.VMEM)
    dma = pltpu.SemaphoreType.DMA
    return pl.pallas_call(
        lambda *refs: gather_kernel(members, *refs),
        name="gather_project",
        out_shape=(
            jax.ShapeDtypeStruct((local, rows, ff), BF16),
            jax.ShapeDtypeStruct((tokens, ff), BF16),
            jax.ShapeDtypeStruct((members - 1, tokens, d), BF16),
            jax.ShapeDtypeStruct((members, *meta.shape), F32),
        ),
        in_specs=[hbm, vmem, hbm, hbm, hbm, hbm],
        out_specs=(hbm, hbm, hbm, vmem),
        scratch_shapes=[
            pltpu.VMEM((steps, rows, F_COLUMNS), F32),
            pltpu.VMEM((steps, rows, F_COLUMNS), F32),
            pltpu.VMEM((members, tokens, X_COLUMNS), BF16),
            pltpu.VMEM((local, rows, X_COLUMNS), BF16),
            pltpu.VMEM((members, local * slots, tokens), BF16),
            pltpu.VMEM((X_RING, 2, X_COLUMNS, F_COLUMNS), BF16),
            pltpu.VMEM((ff // hw, rows, hw), BF16),
            pltpu.VMEM((members - 1, *meta.shape), F32),
            dma((chunks, 2)), dma((chunks, 2)), dma((chunks, 2)), dma((chunks, 2)),
            dma((members - 1,)), dma((members - 1,)), dma((X_RING, 2)), dma((members,)), dma((ff // hw,)),
        ],
        compiler_params=pltpu.CompilerParams(collective_id=0, has_side_effects=True, vmem_limit_bytes=VMEM_BYTES),
    )(x, meta, w_gate, w_up, s_gate, s_up)


def scatter(members, h, hs, metas, w_down, s_down):
    (local, rows, ff), (tokens, d) = h.shape, (hs.shape[0], w_down.shape[2])
    chunks, half = d // Y_COLUMNS, tokens // 2
    slots = rows // members
    hbm, vmem = pl.BlockSpec(memory_space=pl.ANY), pl.BlockSpec(memory_space=pltpu.VMEM)
    dma = pltpu.SemaphoreType.DMA
    return pl.pallas_call(
        lambda *refs: scatter_kernel(members, *refs),
        name="project_scatter",
        out_shape=jax.ShapeDtypeStruct((tokens, d), BF16),
        in_specs=[hbm, vmem, vmem, hbm, hbm],
        out_specs=hbm,
        scratch_shapes=[
            pltpu.VMEM(h.shape, BF16),
            pltpu.VMEM((members, tokens, local * slots), BF16),
            pltpu.VMEM((Y_RING, 2, ff, Y_COLUMNS), BF16),
            pltpu.VMEM((members, local, slots, Y_COLUMNS), BF16),
            pltpu.VMEM((2, 2, tokens, Y_COLUMNS), F32),
            pltpu.VMEM((LAG + 1, tokens, Y_COLUMNS), F32),
            pltpu.VMEM((2, tokens, Y_COLUMNS), BF16),
            pltpu.VMEM((2, 2, tokens, Y_COLUMNS), BF16),
            pltpu.VMEM((chunks, 2, half, Y_COLUMNS), BF16),
            pltpu.VMEM((chunks, 2, tokens, Y_COLUMNS), BF16),
            pltpu.VMEM((2, tokens, Y_COLUMNS), BF16),
            dma((local,)), dma((Y_RING, 2)),
            dma((chunks, 2)), dma((chunks, 2)), dma((chunks, 2)), dma((chunks, 2)), dma((2,)),
        ],
        compiler_params=pltpu.CompilerParams(collective_id=1, has_side_effects=True, vmem_limit_bytes=VMEM_BYTES),
    )(h, hs, metas, w_down, s_down)


def solution(mesh):
    members = mesh.shape["ep"]

    def body(x, expert, slot, gate, w_gate, w_up, w_down, s_gate, s_up, s_down):
        x, expert, slot, gate = (v[0, 0] for v in (x, expert, slot, gate))
        tokens, top = expert.shape
        slots = 5 * tokens * top // (4 * w_gate.shape[0] * members)
        at = jnp.where(slot < slots, expert * slots + slot, -1).astype(F32)
        meta = jnp.concatenate([at, gate.astype(BF16).astype(F32)], 1).T
        h, hs, _, metas = gather(members, x, meta, w_gate, w_up, s_gate, s_up, slots)
        y = scatter(members, h, hs, metas.transpose(0, 2, 1), w_down, s_down)
        return y[None, None]

    tok, exp, rep = P("dp", "ep"), P("ep"), P()
    return jax.shard_map(
        body,
        mesh=mesh,
        in_specs=(tok,) * 4 + (exp,) * 3 + (rep,) * 3,
        out_specs=tok,
        check_vma=False,
    )
```

```python
import jax
import jax.numpy as jnp
from jax import lax
from jax.experimental import pallas as pl
from jax.experimental.pallas import tpu as pltpu
from jax.sharding import PartitionSpec as P

F32, BF16 = jnp.float32, jnp.bfloat16
MESH = pl.DeviceIdType.MESH
VMEM_BYTES = 67_000_000
X_COLUMNS, F_COLUMNS, H_COLUMNS, H_RING, X_RING = 512, 1536, 256, 4, 3
Y_COLUMNS, Y_GROUP, Y_RING, LAG, MARK_ROWS = 256, 5, 3, 3, 16


def dot(a, b):
    return jnp.dot(a, b, preferred_element_type=F32)


def ring(members):
    me = lax.axis_index("ep")
    return me, lax.rem(me + 1, members), lax.rem(me + members - 1, members), lax.rem(me + 2, members)


def greet(*devices):
    barrier = pltpu.get_barrier_semaphore()
    for device in devices:
        pl.semaphore_signal(barrier, inc=1, device_id={"ep": device}, device_id_type=MESH)
    pl.semaphore_wait(barrier, len(devices))


def remote(src, dst, send, recv, device):
    return pltpu.make_async_remote_copy(
        src_ref=src, dst_ref=dst, send_sem=send, recv_sem=recv, device_id={"ep": device}, device_id_type=MESH
    )


def block(i, size):
    return pl.ds(pl.multiple_of(i * size, size), size)


def gather_kernel(
    members, x, expert, slot, gate, w_gate, w_up, s_gate, s_up, h, hs, xg, metas,
    acc_g, acc_u, xbuf, z, onehot, wbuf, hbuf, mbuf,
    s1s, s1r, s2s, s2r, ms, mr, wsem, xsem, hsem,
):
    (tokens, d), local, (_, rows, width) = x.shape, w_gate.shape[0], z.shape
    slots, half, chunks = rows // members, tokens // 2, d // width
    depth, fb = wbuf.shape[0], wbuf.shape[3]
    ff, hw, top = w_gate.shape[2], hbuf.shape[2], expert.shape[0]
    nf = ff // fb
    head, steps = chunks * nf, local * nf
    me, right, left, across = ring(members)
    sides = (right, left)
    mbuf[0, :top] = jnp.where(slot[...] < slots, expert[...] * slots + slot[...], -1).astype(F32)
    mbuf[0, top:] = gate[...].astype(BF16).astype(F32)
    greet(right, left, across)

    def first(k, side):
        return remote(x.at[:, block(k, width)], xg.at[side, :, block(k, width)], s1s.at[k, side], s1r.at[k, side], sides[side])

    def second(k, side):
        part = pl.ds(side * half, half)
        return remote(
            xg.at[side, part, block(k, width)], xg.at[2, part, block(k, width)], s2s.at[k, side], s2r.at[k, side], sides[side]
        )

    def tell(i):
        return remote(mbuf.at[0], mbuf.at[i + 1], ms.at[i], mr.at[i], (right, left, across)[i])

    def relay(k):
        for side in range(2):
            first(k, side).wait_recv()
        for side in range(2):
            second(k, side).start()

        @pl.when(k + 1 < chunks)
        def _():
            for side in range(2):
                first(k + 1, side).start()

    def weights(g, slot, start):
        def copies(gate, up):
            for i, src in enumerate((gate, up)):
                copy = pltpu.make_async_copy(src, wbuf.at[slot, i], wsem.at[slot, i])
                copy.start() if start else copy.wait()

        if not start:
            return copies(s_gate.at[:width, :fb], s_up.at[:width, :fb])

        @pl.when(g < head)
        def _():
            k, f = g // nf, g % nf
            copies(*(s.at[block(k, width), block(f, fb)] for s in (s_gate, s_up)))

        @pl.when((g >= head) & (g < head + chunks * steps))
        def _():
            k, i = (g - head) // steps, (g - head) % steps
            copies(*(w.at[i // nf, block(k, width), block(i % nf, fb)] for w in (w_gate, w_up)))

    def tokens_in(k, source, slot):
        src = x if source == 0 else xg.at[source - 1]
        return pltpu.make_async_copy(src.at[:, block(k, width)], xbuf.at[slot], xsem.at[slot])

    def put(dst, p):
        return pltpu.make_async_copy(hbuf.at[p], dst, hsem.at[p])

    def activate(zz, i, slot, dst, last):
        for j in range(fb // hw):
            part = pl.ds(j * hw, hw)
            g, u = acc_g[i, :, part], acc_u[i, :, part]
            if last:
                g += dot(zz, wbuf[slot, 0, :, part])
                u += dot(zz, wbuf[slot, 1, :, part])
            v = (jax.nn.silu(g) * u).astype(BF16)
            p = (i % nf) * (fb // hw) + j
            c = (i + nf if last else i) * (fb // hw) + j
            if last or c >= H_RING:
                put(hs.at[:, pl.ds(0, hw)], c % H_RING).wait()
            hbuf[c % H_RING] = v
            put(dst.at[:, block(p, hw)], c % H_RING).start()

    def mark(r):
        at = mbuf[r, :top] - (me * local * slots).astype(F32)
        for e in range(local):
            row = (lax.broadcasted_iota(jnp.int32, (slots, tokens), 0) + e * slots).astype(F32)
            hit = at[0:1] == row
            for j in range(1, top):
                hit |= at[j : j + 1] == row
            n = e % (local // 2) * slots
            onehot[r, e // (local // 2), n : n + slots, :] = jnp.where(hit, 1.0, 0.0).astype(BF16)

    for side in range(2):
        first(0, side).start()
    for k in range(members - 1):
        tokens_in(k, 0, k).start()
    for g in range(depth - 1):
        weights(jnp.int32(g), g, True)
    for i in range(members - 1):
        tell(i).start()

    @pl.loop(0, chunks)
    def _(k):
        slot_x = k % members

        @pl.when(k + members - 1 < chunks)
        def _():
            tokens_in(k + members - 1, 0, (k + members - 1) % members).start()

        @pl.when(k == (2 * chunks) // 3)
        def _():
            relay(0)

        @pl.when(k == chunks - members)
        def _():
            for i in range(members - 1):
                tell(i).wait_recv()

        tokens_in(k, 0, slot_x).wait()
        for f in range(nf):
            g = k * nf + f
            slot = g % depth
            weights(g, slot, False)
            weights(g + depth - 1, (g + depth - 1) % depth, True)

            @pl.when(k == 0)
            def _():
                acc_g[f] = dot(xbuf[slot_x], wbuf[slot, 0])
                acc_u[f] = dot(xbuf[slot_x], wbuf[slot, 1])

            @pl.when((k > 0) & (k < chunks - members))
            def _():
                acc_g[f] += dot(xbuf[slot_x], wbuf[slot, 0])
                acc_u[f] += dot(xbuf[slot_x], wbuf[slot, 1])

            @pl.when(k >= chunks - members)
            def _():
                if f == 0:
                    mark(k - (chunks - members))
                acc_g[f] += dot(xbuf[slot_x], wbuf[slot, 0])
                acc_u[f] += dot(xbuf[slot_x], wbuf[slot, 1])

    for f in range(nf):
        activate(None, f, 0, hs, False)

    for side in range(2):
        second(jnp.int32(0), side).wait_recv()
    for r in range(members):
        tokens_in(0, r, r).start()

    @pl.loop(0, 2 * chunks)
    def _(t):
        k, j = t // 2, t % 2

        @pl.when(j == 0)
        def _():
            for r in range(members):
                tokens_in(k, r, r).wait()

        for r in range(members):
            v = dot(onehot[r, j], xbuf[r]).astype(BF16)
            z[:, r * slots : (r + 1) * slots, :] = v.reshape(local // 2, slots, width)

        @pl.loop(0, steps // 2)
        def _(s):
            i = j * (steps // 2) + s
            g = head + k * steps + i
            slot = g % depth

            @pl.when((i == steps // 5) & (k + 1 < chunks))
            def _():
                relay(k + 1)

            @pl.when((i == (4 * steps) // 5) & (k + 1 < chunks))
            def _():
                for side in range(2):
                    second(k + 1, side).wait_recv()
                for r in range(members):
                    tokens_in(k + 1, r, r).start()

            weights(g, slot, False)
            weights(g + depth - 1, (g + depth - 1) % depth, True)
            e = s // nf

            @pl.when(k == 0)
            def _():
                acc_g[i] = dot(z[e], wbuf[slot, 0])
                acc_u[i] = dot(z[e], wbuf[slot, 1])

            @pl.when((k > 0) & (k < chunks - 1))
            def _():
                acc_g[i] += dot(z[e], wbuf[slot, 0])
                acc_u[i] += dot(z[e], wbuf[slot, 1])

            @pl.when(k == chunks - 1)
            def _():
                activate(z[e], i, slot, h.at[i // nf], True)

    for p in range(H_RING):
        put(hs.at[:, pl.ds(0, hw)], p).wait()
    for i in range(members - 1):
        tell(i).wait_send()

    @pl.loop(0, chunks)
    def _(k):
        for side in range(2):
            first(k, side).wait_send()
            second(k, side).wait_send()

    metas[...] = mbuf[...]


def scatter_kernel(
    members, h, hs, metas, w_down, s_down, y,
    hbuf, comb, wbuf, outs, pend, own, abuf, bbuf, arecv, brecv, ybuf,
    hsem, wsem, a_s, a_r, b_s, b_r, ysem,
):
    (local, rows, ff), width, d = h.shape, wbuf.shape[3], y.shape[1]
    tokens, top = hs.shape[0], metas.shape[1] // 2
    slots, half, chunks = rows // members, tokens // 2, d // width
    (depth, group), lag = wbuf.shape[:2], own.shape[0] - 1
    groups = local // group
    steps = groups + 1
    me, right, left, _ = ring(members)
    sides = (right, left)
    greet(right, left)

    def weights(g, slot, start):
        n, p = g // steps, g % steps

        def go(copy):
            copy.start() if start else copy.wait()

        @pl.when((p < groups) & (n < chunks))
        def _():
            for i in range(group):
                go(pltpu.make_async_copy(w_down.at[group * p + i, :, block(n, width)], wbuf.at[slot, i], wsem.at[slot, i]))

        @pl.when((p == groups) & (n < chunks))
        def _():
            go(pltpu.make_async_copy(s_down.at[:, block(n, width)], wbuf.at[slot, 0], wsem.at[slot, 0]))

    def take(e):
        return pltpu.make_async_copy(h.at[e], hbuf.at[e], hsem.at[e])

    def across(n, side):
        return remote(abuf.at[n % 2, pl.ds(side * half, half)], arecv.at[n, side], a_s.at[n, side], a_r.at[n, side], sides[side])

    def beside(n, side):
        return remote(bbuf.at[n % 2, side], brecv.at[n, side], b_s.at[n, side], b_r.at[n, side], sides[side])

    def put(n):
        return pltpu.make_async_copy(ybuf.at[n % 2], y.at[:, block(n, width)], ysem.at[n % 2])

    for e in range(local):
        take(e).start()
    for g in range(depth - 1):
        weights(jnp.int32(g), g, True)

    def mark(r):
        m = metas[r].T
        at, gate = m[:, :top] - (me * local * slots).astype(F32), m[:, top:]
        row = lax.broadcasted_iota(jnp.int32, (MARK_ROWS, local * slots), 1).astype(F32)
        for t in range(0, tokens, MARK_ROWS):
            v = jnp.zeros(row.shape, F32)
            for j in range(top):
                v = jnp.where(at[t : t + MARK_ROWS, j : j + 1] == row, gate[t : t + MARK_ROWS, j : j + 1], v)
            comb[r, t : t + MARK_ROWS] = v.astype(BF16)

    mark(3)
    mark(2)

    @pl.loop(0, chunks + lag)
    def _(n):
        @pl.when(n < chunks)
        def _():
            @pl.loop(0, groups)
            def _(p):
                g = n * steps + p
                slot = g % depth

                @pl.when(n == 0)
                def _():
                    for i in range(group):
                        take(group * p + i).wait()

                weights(g, slot, False)
                weights(g + depth - 1, (g + depth - 1) % depth, True)
                for i in range(group):
                    v = dot(hbuf[group * p + i], wbuf[slot, i]).astype(BF16)
                    outs[:, group * p + i] = v.reshape(members, slots, width)

            def term(r):
                return dot(comb[r], outs[r].reshape(local * slots, width))

            @pl.when(n >= 2)
            def _():
                for side in range(2):
                    across(n - 2, side).wait_send()

            abuf[n % 2] = term(3).astype(BF16)
            for side in range(2):
                across(n, side).start()

            @pl.when(n == 0)
            def _():
                mark(1)
                mark(0)

            g = n * steps + groups
            slot = g % depth
            weights(g, slot, False)
            weights(g + depth - 1, (g + depth - 1) % depth, True)
            pend[n % 2, 0] = term(2)
            pend[n % 2, 1] = term(1)
            own[n % (lag + 1)] = term(0) + dot(hs[...], wbuf[slot, 0])

        @pl.when((n >= 1) & (n <= chunks))
        def _():
            m = n - 1
            for side in range(2):
                across(m, side).wait_recv()

            @pl.when(m >= 2)
            def _():
                for side in range(2):
                    beside(m - 2, side).wait_send()

            for side in range(2):
                mine, other = pl.ds(side * half, half), pl.ds((1 - side) * half, half)
                v = pend[m % 2, side, mine] + arecv[m, side].astype(F32)
                bbuf[m % 2, side, mine] = v.astype(BF16)
                bbuf[m % 2, side, other] = pend[m % 2, side, other].astype(BF16)
                beside(m, side).start()

        @pl.when(n >= lag)
        def _():
            q = n - lag
            for side in range(2):
                beside(q, side).wait_recv()

            @pl.when(q >= 2)
            def _():
                put(q - 2).wait()

            ybuf[q % 2] = (own[q % (lag + 1)] + brecv[q, 0].astype(F32) + brecv[q, 1].astype(F32)).astype(BF16)
            put(q).start()

    for n in range(chunks - 2, chunks):
        put(jnp.int32(n)).wait()
        for side in range(2):
            across(jnp.int32(n), side).wait_send()
            beside(jnp.int32(n), side).wait_send()


def gather(members, x, expert, slot, gate, w_gate, w_up, s_gate, s_up, slots):
    (tokens, d), (local, _, ff) = x.shape, w_gate.shape
    rows, chunks, hw, top = members * slots, d // X_COLUMNS, H_COLUMNS, expert.shape[0]
    steps = local * ff // F_COLUMNS
    hbm, vmem = pl.BlockSpec(memory_space=pl.ANY), pl.BlockSpec(memory_space=pltpu.VMEM)
    dma = pltpu.SemaphoreType.DMA
    return pl.pallas_call(
        lambda *refs: gather_kernel(members, *refs),
        name="gather_project",
        out_shape=(
            jax.ShapeDtypeStruct((local, rows, ff), BF16),
            jax.ShapeDtypeStruct((tokens, ff), BF16),
            jax.ShapeDtypeStruct((members - 1, tokens, d), BF16),
            jax.ShapeDtypeStruct((members, 2 * top, tokens), F32),
        ),
        in_specs=[hbm, vmem, vmem, vmem, hbm, hbm, hbm, hbm],
        out_specs=(hbm, hbm, hbm, vmem),
        scratch_shapes=[
            pltpu.VMEM((steps, rows, F_COLUMNS), F32),
            pltpu.VMEM((steps, rows, F_COLUMNS), F32),
            pltpu.VMEM((members, tokens, X_COLUMNS), BF16),
            pltpu.VMEM((local // 2, rows, X_COLUMNS), BF16),
            pltpu.VMEM((members, 2, local // 2 * slots, tokens), BF16),
            pltpu.VMEM((X_RING, 2, X_COLUMNS, F_COLUMNS), BF16),
            pltpu.VMEM((H_RING, rows, hw), BF16),
            pltpu.VMEM((members, 2 * top, tokens), F32),
            dma((chunks, 2)), dma((chunks, 2)), dma((chunks, 2)), dma((chunks, 2)),
            dma((members - 1,)), dma((members - 1,)), dma((X_RING, 2)), dma((members,)), dma((H_RING,)),
        ],
        compiler_params=pltpu.CompilerParams(collective_id=0, has_side_effects=True, vmem_limit_bytes=VMEM_BYTES),
    )(x, expert, slot, gate, w_gate, w_up, s_gate, s_up)


def scatter(members, h, hs, metas, w_down, s_down):
    (local, rows, ff), (tokens, d) = h.shape, (hs.shape[0], w_down.shape[2])
    chunks, half = d // Y_COLUMNS, tokens // 2
    slots = rows // members
    hbm, vmem = pl.BlockSpec(memory_space=pl.ANY), pl.BlockSpec(memory_space=pltpu.VMEM)
    dma = pltpu.SemaphoreType.DMA
    return pl.pallas_call(
        lambda *refs: scatter_kernel(members, *refs),
        name="project_scatter",
        out_shape=jax.ShapeDtypeStruct((tokens, d), BF16),
        in_specs=[hbm, vmem, vmem, hbm, hbm],
        out_specs=hbm,
        scratch_shapes=[
            pltpu.VMEM(h.shape, BF16),
            pltpu.VMEM((members, tokens, local * slots), BF16),
            pltpu.VMEM((Y_RING, Y_GROUP, ff, Y_COLUMNS), BF16),
            pltpu.VMEM((members, local, slots, Y_COLUMNS), BF16),
            pltpu.VMEM((2, 2, tokens, Y_COLUMNS), F32),
            pltpu.VMEM((LAG + 1, tokens, Y_COLUMNS), F32),
            pltpu.VMEM((2, tokens, Y_COLUMNS), BF16),
            pltpu.VMEM((2, 2, tokens, Y_COLUMNS), BF16),
            pltpu.VMEM((chunks, 2, half, Y_COLUMNS), BF16),
            pltpu.VMEM((chunks, 2, tokens, Y_COLUMNS), BF16),
            pltpu.VMEM((2, tokens, Y_COLUMNS), BF16),
            dma((local,)), dma((Y_RING, Y_GROUP)),
            dma((chunks, 2)), dma((chunks, 2)), dma((chunks, 2)), dma((chunks, 2)), dma((2,)),
        ],
        compiler_params=pltpu.CompilerParams(collective_id=1, has_side_effects=True, vmem_limit_bytes=VMEM_BYTES),
    )(h, hs, metas, w_down, s_down)


def solution(mesh):
    members = mesh.shape["ep"]

    def body(x, expert, slot, gate, w_gate, w_up, w_down, s_gate, s_up, s_down):
        x, expert, slot, gate = (v[0, 0] for v in (x, expert, slot, gate))
        tokens, top = expert.shape
        slots = 5 * tokens * top // (4 * w_gate.shape[0] * members)
        h, hs, _, metas = gather(members, x, expert.T, slot.T, gate.T, w_gate, w_up, s_gate, s_up, slots)
        y = scatter(members, h, hs, metas, w_down, s_down)
        return y[None, None]

    tok, exp, rep = P("dp", "ep"), P("ep"), P()
    return jax.shard_map(
        body,
        mesh=mesh,
        in_specs=(tok,) * 4 + (exp,) * 3 + (rep,) * 3,
        out_specs=tok,
        check_vma=False,
    )
```

```python
import jax
import jax.numpy as jnp
from jax import lax
from jax.experimental import pallas as pl
from jax.experimental.pallas import tpu as pltpu
from jax.sharding import PartitionSpec as P

F32, BF16 = jnp.float32, jnp.bfloat16
MESH = pl.DeviceIdType.MESH
VMEM_BYTES = 67_000_000
X_COLUMNS, F_COLUMNS, H_COLUMNS, H_RING, X_RING = 512, 1536, 256, 4, 3
Y_COLUMNS, Y_GROUP, Y_RING, LAG, MARK_ROWS = 256, 5, 3, 3, 16


def dot(a, b):
    return jnp.dot(a, b, preferred_element_type=F32)


def ring(members):
    me = lax.axis_index("ep")
    return me, lax.rem(me + 1, members), lax.rem(me + members - 1, members), lax.rem(me + 2, members)


def greet(*devices):
    barrier = pltpu.get_barrier_semaphore()
    for device in devices:
        pl.semaphore_signal(barrier, inc=1, device_id={"ep": device}, device_id_type=MESH)
    pl.semaphore_wait(barrier, len(devices))


def remote(src, dst, send, recv, device):
    return pltpu.make_async_remote_copy(
        src_ref=src, dst_ref=dst, send_sem=send, recv_sem=recv, device_id={"ep": device}, device_id_type=MESH
    )


def block(i, size):
    return pl.ds(pl.multiple_of(i * size, size), size)


def gather_kernel(
    members, x, expert, slot, gate, w_gate, w_up, s_gate, s_up, h, hs, xg, metas,
    acc_g, acc_u, xbuf, z, onehot, wbuf, hbuf, mbuf,
    s1s, s1r, s2s, s2r, ms, mr, wsem, xsem, hsem,
):
    (tokens, d), local, (_, rows, width) = x.shape, w_gate.shape[0], z.shape
    slots, half, chunks = rows // members, tokens // 2, d // width
    depth, fb = wbuf.shape[0], wbuf.shape[3]
    ff, hw, top = w_gate.shape[2], hbuf.shape[2], expert.shape[0]
    nf = ff // fb
    head, steps = chunks * nf, local * nf
    me, right, left, across = ring(members)
    sides = (right, left)
    mbuf[0, :top] = jnp.where(slot[...] < slots, expert[...] * slots + slot[...], -1).astype(F32)
    mbuf[0, top:] = gate[...].astype(BF16).astype(F32)
    greet(right, left, across)

    def first(k, side):
        return remote(x.at[:, block(k, width)], xg.at[side, :, block(k, width)], s1s.at[k, side], s1r.at[k, side], sides[side])

    def second(k, side):
        part = pl.ds(side * half, half)
        return remote(
            xg.at[side, part, block(k, width)], xg.at[2, part, block(k, width)], s2s.at[k, side], s2r.at[k, side], sides[side]
        )

    def tell(i):
        return remote(mbuf.at[0], mbuf.at[i + 1], ms.at[i], mr.at[i], (right, left, across)[i])

    def relay(k):
        for side in range(2):
            first(k, side).wait_recv()
        for side in range(2):
            second(k, side).start()

    def send(k):
        for side in range(2):
            first(k, side).start()

    def weights(g, slot, start):
        def copies(gate, up):
            for i, src in enumerate((gate, up)):
                copy = pltpu.make_async_copy(src, wbuf.at[slot, i], wsem.at[slot, i])
                copy.start() if start else copy.wait()

        if not start:
            return copies(s_gate.at[:width, :fb], s_up.at[:width, :fb])

        @pl.when(g < head)
        def _():
            k, f = g // nf, g % nf
            copies(*(s.at[block(k, width), block(f, fb)] for s in (s_gate, s_up)))

        @pl.when((g >= head) & (g < head + chunks * steps))
        def _():
            k, i = (g - head) // steps, (g - head) % steps
            copies(*(w.at[i // nf, block(k, width), block(i % nf, fb)] for w in (w_gate, w_up)))

    def tokens_in(k, source, slot):
        src = x if source == 0 else xg.at[source - 1]
        return pltpu.make_async_copy(src.at[:, block(k, width)], xbuf.at[slot], xsem.at[slot])

    def put(dst, p):
        return pltpu.make_async_copy(hbuf.at[p], dst, hsem.at[p])

    def activate(zz, i, slot, dst, last):
        for j in range(fb // hw):
            part = pl.ds(j * hw, hw)
            g, u = acc_g[i, :, part], acc_u[i, :, part]
            if last:
                g += dot(zz, wbuf[slot, 0, :, part])
                u += dot(zz, wbuf[slot, 1, :, part])
            v = (jax.nn.silu(g) * u).astype(BF16)
            p = (i % nf) * (fb // hw) + j
            c = (i + nf if last else i) * (fb // hw) + j
            if last or c >= H_RING:
                put(hs.at[:, pl.ds(0, hw)], c % H_RING).wait()
            hbuf[c % H_RING] = v
            put(dst.at[:, block(p, hw)], c % H_RING).start()

    def mark(r):
        at = mbuf[r, :top] - (me * local * slots).astype(F32)
        for e in range(local):
            row = (lax.broadcasted_iota(jnp.int32, (slots, tokens), 0) + e * slots).astype(F32)
            hit = at[0:1] == row
            for j in range(1, top):
                hit |= at[j : j + 1] == row
            n = e % (local // 2) * slots
            onehot[r, e // (local // 2), n : n + slots, :] = jnp.where(hit, 1.0, 0.0).astype(BF16)

    send(0)
    for k in range(members - 1):
        tokens_in(k, 0, k).start()
    for g in range(depth - 1):
        weights(jnp.int32(g), g, True)
    for i in range(members - 1):
        tell(i).start()

    @pl.loop(0, chunks)
    def _(k):
        slot_x = k % members

        @pl.when(k + members - 1 < chunks)
        def _():
            tokens_in(k + members - 1, 0, (k + members - 1) % members).start()

        @pl.when(k == chunks - 3)
        def _():
            relay(0)

        @pl.when(k == chunks - 1)
        def _():
            send(1)

        @pl.when(k == chunks - members)
        def _():
            for i in range(members - 1):
                tell(i).wait_recv()

        tokens_in(k, 0, slot_x).wait()
        for f in range(nf):
            g = k * nf + f
            slot = g % depth
            weights(g, slot, False)
            weights(g + depth - 1, (g + depth - 1) % depth, True)

            @pl.when(k == 0)
            def _():
                acc_g[f] = dot(xbuf[slot_x], wbuf[slot, 0])
                acc_u[f] = dot(xbuf[slot_x], wbuf[slot, 1])

            @pl.when((k > 0) & (k < chunks - members))
            def _():
                acc_g[f] += dot(xbuf[slot_x], wbuf[slot, 0])
                acc_u[f] += dot(xbuf[slot_x], wbuf[slot, 1])

            @pl.when(k >= chunks - members)
            def _():
                if f == 0:
                    mark(k - (chunks - members))
                acc_g[f] += dot(xbuf[slot_x], wbuf[slot, 0])
                acc_u[f] += dot(xbuf[slot_x], wbuf[slot, 1])

    for f in range(nf):
        activate(None, f, 0, hs, False)

    for side in range(2):
        second(jnp.int32(0), side).wait_recv()
    for r in range(members):
        tokens_in(0, r, r).start()

    @pl.loop(0, 2 * chunks)
    def _(t):
        k, j = t // 2, t % 2

        @pl.when(j == 0)
        def _():
            for r in range(members):
                tokens_in(k, r, r).wait()

        for r in range(members):
            v = dot(onehot[r, j], xbuf[r]).astype(BF16)
            z[:, r * slots : (r + 1) * slots, :] = v.reshape(local // 2, slots, width)

        @pl.loop(0, steps // 2)
        def _(s):
            i = j * (steps // 2) + s
            g = head + k * steps + i
            slot = g % depth

            @pl.when((i == 3 * steps // 10) & (k + 1 < chunks))
            def _():
                relay(k + 1)

            @pl.when((i == 6 * steps // 10) & (k + 2 < chunks))
            def _():
                send(k + 2)

            @pl.when((i == (4 * steps) // 5) & (k + 1 < chunks))
            def _():
                for side in range(2):
                    second(k + 1, side).wait_recv()
                for r in range(members):
                    tokens_in(k + 1, r, r).start()

            weights(g, slot, False)
            weights(g + depth - 1, (g + depth - 1) % depth, True)
            e = s // nf

            @pl.when(k == 0)
            def _():
                acc_g[i] = dot(z[e], wbuf[slot, 0])
                acc_u[i] = dot(z[e], wbuf[slot, 1])

            @pl.when((k > 0) & (k < chunks - 1))
            def _():
                acc_g[i] += dot(z[e], wbuf[slot, 0])
                acc_u[i] += dot(z[e], wbuf[slot, 1])

            @pl.when(k == chunks - 1)
            def _():
                activate(z[e], i, slot, h.at[i // nf], True)

    for p in range(H_RING):
        put(hs.at[:, pl.ds(0, hw)], p).wait()
    for i in range(members - 1):
        tell(i).wait_send()

    @pl.loop(0, chunks)
    def _(k):
        for side in range(2):
            first(k, side).wait_send()
            second(k, side).wait_send()

    metas[...] = mbuf[...]


def scatter_kernel(
    members, h, hs, metas, w_down, s_down, y,
    hbuf, comb, wbuf, outs, pend, own, abuf, bbuf, arecv, brecv, ybuf,
    hsem, wsem, a_s, a_r, b_s, b_r, ysem,
):
    (local, rows, ff), width, d = h.shape, wbuf.shape[3], y.shape[1]
    tokens, top = hs.shape[0], metas.shape[1] // 2
    slots, half, chunks = rows // members, tokens // 2, d // width
    (depth, group), lag = wbuf.shape[:2], own.shape[0] - 1
    groups = local // group
    steps = groups + 1
    me, right, left, _ = ring(members)
    sides = (right, left)
    greet(right, left)

    def weights(g, slot, start):
        n, p = g // steps, g % steps

        def go(copy):
            copy.start() if start else copy.wait()

        @pl.when((p < groups) & (n < chunks))
        def _():
            for i in range(group):
                go(pltpu.make_async_copy(w_down.at[group * p + i, :, block(n, width)], wbuf.at[slot, i], wsem.at[slot, i]))

        @pl.when((p == groups) & (n < chunks))
        def _():
            go(pltpu.make_async_copy(s_down.at[:, block(n, width)], wbuf.at[slot, 0], wsem.at[slot, 0]))

    def take(e):
        return pltpu.make_async_copy(h.at[e], hbuf.at[e], hsem.at[e])

    def across(n, side):
        return remote(abuf.at[n % 2, pl.ds(side * half, half)], arecv.at[n, side], a_s.at[n, side], a_r.at[n, side], sides[side])

    def beside(n, side):
        return remote(bbuf.at[n % 2, side], brecv.at[n, side], b_s.at[n, side], b_r.at[n, side], sides[side])

    def put(n):
        return pltpu.make_async_copy(ybuf.at[n % 2], y.at[:, block(n, width)], ysem.at[n % 2])

    for e in range(local):
        take(e).start()
    for g in range(depth - 1):
        weights(jnp.int32(g), g, True)

    def mark(r):
        m = metas[r].T
        at, gate = m[:, :top] - (me * local * slots).astype(F32), m[:, top:]
        row = lax.broadcasted_iota(jnp.int32, (MARK_ROWS, local * slots), 1).astype(F32)
        for t in range(0, tokens, MARK_ROWS):
            v = jnp.zeros(row.shape, F32)
            for j in range(top):
                v = jnp.where(at[t : t + MARK_ROWS, j : j + 1] == row, gate[t : t + MARK_ROWS, j : j + 1], v)
            comb[r, t : t + MARK_ROWS] = v.astype(BF16)

    mark(3)
    mark(2)

    @pl.loop(0, chunks + lag)
    def _(n):
        @pl.when(n < chunks)
        def _():
            @pl.loop(0, groups)
            def _(p):
                g = n * steps + p
                slot = g % depth

                @pl.when(n == 0)
                def _():
                    for i in range(group):
                        take(group * p + i).wait()

                weights(g, slot, False)
                weights(g + depth - 1, (g + depth - 1) % depth, True)

                def project():
                    for i in range(group):
                        v = dot(hbuf[group * p + i], wbuf[slot, i]).astype(BF16)
                        outs[:, group * p + i] = v.reshape(members, slots, width)

                early = (n == 0) & (p < 2)

                @pl.when(early)
                def _():
                    mark(1 - p)
                    project()

                @pl.when(jnp.logical_not(early))
                def _():
                    project()

            def term(r):
                return dot(comb[r], outs[r].reshape(local * slots, width))

            @pl.when(n >= 2)
            def _():
                for side in range(2):
                    across(n - 2, side).wait_send()

            abuf[n % 2] = term(3).astype(BF16)
            for side in range(2):
                across(n, side).start()

            g = n * steps + groups
            slot = g % depth
            weights(g, slot, False)
            weights(g + depth - 1, (g + depth - 1) % depth, True)
            pend[n % 2, 0] = term(2)
            pend[n % 2, 1] = term(1)
            own[n % (lag + 1)] = term(0) + dot(hs[...], wbuf[slot, 0])

        @pl.when((n >= 1) & (n <= chunks))
        def _():
            m = n - 1
            for side in range(2):
                across(m, side).wait_recv()

            @pl.when(m >= 2)
            def _():
                for side in range(2):
                    beside(m - 2, side).wait_send()

            for side in range(2):
                mine, other = pl.ds(side * half, half), pl.ds((1 - side) * half, half)
                v = pend[m % 2, side, mine] + arecv[m, side].astype(F32)
                bbuf[m % 2, side, mine] = v.astype(BF16)
                bbuf[m % 2, side, other] = pend[m % 2, side, other].astype(BF16)
                beside(m, side).start()

        @pl.when(n >= lag)
        def _():
            q = n - lag
            for side in range(2):
                beside(q, side).wait_recv()

            @pl.when(q >= 2)
            def _():
                put(q - 2).wait()

            ybuf[q % 2] = (own[q % (lag + 1)] + brecv[q, 0].astype(F32) + brecv[q, 1].astype(F32)).astype(BF16)
            put(q).start()

    for n in range(chunks - 2, chunks):
        put(jnp.int32(n)).wait()
        for side in range(2):
            across(jnp.int32(n), side).wait_send()
            beside(jnp.int32(n), side).wait_send()


def gather(members, x, expert, slot, gate, w_gate, w_up, s_gate, s_up, slots):
    (tokens, d), (local, _, ff) = x.shape, w_gate.shape
    rows, chunks, hw, top = members * slots, d // X_COLUMNS, H_COLUMNS, expert.shape[0]
    steps = local * ff // F_COLUMNS
    hbm, vmem = pl.BlockSpec(memory_space=pl.ANY), pl.BlockSpec(memory_space=pltpu.VMEM)
    dma = pltpu.SemaphoreType.DMA
    return pl.pallas_call(
        lambda *refs: gather_kernel(members, *refs),
        name="gather_project",
        out_shape=(
            jax.ShapeDtypeStruct((local, rows, ff), BF16),
            jax.ShapeDtypeStruct((tokens, ff), BF16),
            jax.ShapeDtypeStruct((members - 1, tokens, d), BF16),
            jax.ShapeDtypeStruct((members, 2 * top, tokens), F32),
        ),
        in_specs=[hbm, vmem, vmem, vmem, hbm, hbm, hbm, hbm],
        out_specs=(hbm, hbm, hbm, vmem),
        scratch_shapes=[
            pltpu.VMEM((steps, rows, F_COLUMNS), F32),
            pltpu.VMEM((steps, rows, F_COLUMNS), F32),
            pltpu.VMEM((members, tokens, X_COLUMNS), BF16),
            pltpu.VMEM((local // 2, rows, X_COLUMNS), BF16),
            pltpu.VMEM((members, 2, local // 2 * slots, tokens), BF16),
            pltpu.VMEM((X_RING, 2, X_COLUMNS, F_COLUMNS), BF16),
            pltpu.VMEM((H_RING, rows, hw), BF16),
            pltpu.VMEM((members, 2 * top, tokens), F32),
            dma((chunks, 2)), dma((chunks, 2)), dma((chunks, 2)), dma((chunks, 2)),
            dma((members - 1,)), dma((members - 1,)), dma((X_RING, 2)), dma((members,)), dma((H_RING,)),
        ],
        compiler_params=pltpu.CompilerParams(collective_id=0, has_side_effects=True, vmem_limit_bytes=VMEM_BYTES),
    )(x, expert, slot, gate, w_gate, w_up, s_gate, s_up)


def scatter(members, h, hs, metas, w_down, s_down):
    (local, rows, ff), (tokens, d) = h.shape, (hs.shape[0], w_down.shape[2])
    chunks, half = d // Y_COLUMNS, tokens // 2
    slots = rows // members
    hbm, vmem = pl.BlockSpec(memory_space=pl.ANY), pl.BlockSpec(memory_space=pltpu.VMEM)
    dma = pltpu.SemaphoreType.DMA
    return pl.pallas_call(
        lambda *refs: scatter_kernel(members, *refs),
        name="project_scatter",
        out_shape=jax.ShapeDtypeStruct((tokens, d), BF16),
        in_specs=[hbm, vmem, vmem, hbm, hbm],
        out_specs=hbm,
        scratch_shapes=[
            pltpu.VMEM(h.shape, BF16),
            pltpu.VMEM((members, tokens, local * slots), BF16),
            pltpu.VMEM((Y_RING, Y_GROUP, ff, Y_COLUMNS), BF16),
            pltpu.VMEM((members, local, slots, Y_COLUMNS), BF16),
            pltpu.VMEM((2, 2, tokens, Y_COLUMNS), F32),
            pltpu.VMEM((LAG + 1, tokens, Y_COLUMNS), F32),
            pltpu.VMEM((2, tokens, Y_COLUMNS), BF16),
            pltpu.VMEM((2, 2, tokens, Y_COLUMNS), BF16),
            pltpu.VMEM((chunks, 2, half, Y_COLUMNS), BF16),
            pltpu.VMEM((chunks, 2, tokens, Y_COLUMNS), BF16),
            pltpu.VMEM((2, tokens, Y_COLUMNS), BF16),
            dma((local,)), dma((Y_RING, Y_GROUP)),
            dma((chunks, 2)), dma((chunks, 2)), dma((chunks, 2)), dma((chunks, 2)), dma((2,)),
        ],
        compiler_params=pltpu.CompilerParams(collective_id=1, has_side_effects=True, vmem_limit_bytes=VMEM_BYTES),
    )(h, hs, metas, w_down, s_down)


def solution(mesh):
    members = mesh.shape["ep"]

    def body(x, expert, slot, gate, w_gate, w_up, w_down, s_gate, s_up, s_down):
        x, expert, slot, gate = (v[0, 0] for v in (x, expert, slot, gate))
        tokens, top = expert.shape
        slots = 5 * tokens * top // (4 * w_gate.shape[0] * members)
        h, hs, _, metas = gather(members, x, expert.T, slot.T, gate.T, w_gate, w_up, s_gate, s_up, slots)
        y = scatter(members, h, hs, metas, w_down, s_down)
        return y[None, None]

    tok, exp, rep = P("dp", "ep"), P("ep"), P()
    return jax.shard_map(
        body,
        mesh=mesh,
        in_specs=(tok,) * 4 + (exp,) * 3 + (rep,) * 3,
        out_specs=tok,
        check_vma=False,
    )
```
